128 devices in a mesh: dp: 4 (over z), col: 4 (over y), fsdp: 8 (over x, core).
Axes of the slice: x: 4, y: 4, z: 4, core: 2. Of those that a mesh axis runs over, the one named last changes fastest.
Arguments:
- x_act: bfloat16 [524288, 288], P(('dp', 'col', 'fsdp'))
- dy_out: bfloat16 [524288, 288], P(('dp', 'col', 'fsdp'))
- w_gate: bfloat16 [288, 768], P(None, ('col', 'fsdp'))
- w_up: bfloat16 [288, 768], P(None, ('col', 'fsdp'))
- w_down: bfloat16 [768, 288], P(('col', 'fsdp'))
- v_gate: bfloat16 [288, 768], P(None, ('col', 'fsdp'))
- v_up: bfloat16 [288, 768], P(None, ('col', 'fsdp'))
- v_down: bfloat16 [768, 288], P(('col', 'fsdp'))
- g_next: float32 [128, 3, 288, 768], P(('dp', 'col', 'fsdp'))
Outputs:
- output 1: bfloat16 [524288, 288], P(('dp', 'col', 'fsdp'))
- output 2: float32 [3, 288, 768], P(None, None, ('col', 'fsdp'))
- output 3: float32 [128, 3, 288, 768], P(('dp', 'col', 'fsdp'))
- output 4: bfloat16 [288, 768], replicated
- output 5: bfloat16 [288, 768], replicated
- output 6: bfloat16 [768, 288], replicated
All inputs are finite; a program needn't handle non-finite values.
Results may differ from the reference program's by a relative error of at most 0.0145327.
Values are sent between devices in bfloat16 or wider.
A program may use at most 1 GiB of HBM per device.

```python
import jax
import jax.numpy as jnp
from jax import lax

D_MODEL = 288
D_FF = 768
TOKENS_DEV = 4096
N_DEVICES = 128


def draw_normal(key, shape, scaling):
    return jax.random.normal(key, shape, jnp.float32) * scaling


def setup_inputs(seed: int = 0) -> dict:
    keys = jax.random.split(jax.random.key(seed), 9)
    all_rows = N_DEVICES * TOKENS_DEV
    model_scale = D_MODEL ** -0.5
    hidden_scale = D_FF ** -0.5
    return {
        'x_act': draw_normal(keys[0], (all_rows, D_MODEL), 1.0).astype(jnp.bfloat16),
        'dy_out': draw_normal(keys[1], (all_rows, D_MODEL), 1.0).astype(jnp.bfloat16),
        'w_gate': draw_normal(keys[2], (D_MODEL, D_FF), model_scale).astype(jnp.bfloat16),
        'w_up': draw_normal(keys[3], (D_MODEL, D_FF), model_scale).astype(jnp.bfloat16),
        'w_down': draw_normal(keys[4], (D_FF, D_MODEL), hidden_scale).astype(jnp.bfloat16),
        'v_gate': draw_normal(keys[5], (D_MODEL, D_FF), model_scale).astype(jnp.bfloat16),
        'v_up': draw_normal(keys[6], (D_MODEL, D_FF), model_scale).astype(jnp.bfloat16),
        'v_down': draw_normal(keys[7], (D_FF, D_MODEL), hidden_scale).astype(jnp.bfloat16),
        'g_next': draw_normal(keys[8], (N_DEVICES, 3, D_MODEL, D_FF), 1.0),
    }


def reference(x_act, dy_out, w_gate, w_up, w_down, v_gate, v_up, v_down, g_next):
    x_dev = x_act.reshape(N_DEVICES, TOKENS_DEV, D_MODEL)
    dy_dev = dy_out.reshape(N_DEVICES, TOKENS_DEV, D_MODEL)

    def one_device(operands):
        x_loc, dy_loc = operands
        pre_gate = jnp.dot(x_loc, w_gate, preferred_element_type=jnp.float32)
        pre_up = jnp.dot(x_loc, w_up, preferred_element_type=jnp.float32)
        sig_gate = jax.nn.sigmoid(pre_gate)
        act_gate = pre_gate * sig_gate
        hidden = (act_gate * pre_up).astype(jnp.bfloat16)
        d_hidden = jnp.dot(dy_loc, w_down.T, preferred_element_type=jnp.float32)
        d_gate = (d_hidden * pre_up * sig_gate * (1.0 + pre_gate * (1.0 - sig_gate))).astype(jnp.bfloat16)
        d_up = (d_hidden * act_gate).astype(jnp.bfloat16)
        dx_loc = (jnp.dot(d_gate, w_gate.T, preferred_element_type=jnp.float32)
                  + jnp.dot(d_up, w_up.T, preferred_element_type=jnp.float32)).astype(jnp.bfloat16)
        grad_gate = jnp.dot(x_loc.T, d_gate, preferred_element_type=jnp.float32)
        grad_up = jnp.dot(x_loc.T, d_up, preferred_element_type=jnp.float32)
        grad_down_t = jnp.dot(dy_loc.T, hidden, preferred_element_type=jnp.float32)
        return dx_loc, jnp.stack([grad_gate, grad_up, grad_down_t])

    dx_dev, dw_local = lax.map(one_device, (x_dev, dy_dev))
    dx_in = dx_dev.reshape(N_DEVICES * TOKENS_DEV, D_MODEL)
    dw_next = jnp.sum(g_next.astype(jnp.bfloat16).astype(jnp.float32), axis=0)
    return dx_in, dw_next, dw_local, v_gate, v_up, v_down
```

```python
import functools

import jax
import jax.numpy as jnp
from jax import lax
from jax.experimental import pallas as pl
from jax.experimental.pallas import tpu as pltpu
from jax.sharding import PartitionSpec as P

ALL_AXES = ('dp', 'col', 'fsdp')
FSDP_AXES = ('col', 'fsdp')
F32, BF16 = jnp.float32, jnp.bfloat16
D, F, T = 288, 768, 4096
SH = 24
PK = 896
LA = 384
TB = 512
OFFS = (1, 3, 2)
MESH = pl.DeviceIdType.MESH


class Where:
    def __init__(self):
        self.z = lax.axis_index('dp')
        self.y = lax.axis_index('col')
        f = lax.axis_index('fsdp')
        self.x = lax.div(f, 2)
        self.c = lax.rem(f, 2)

    def xm(self, d):
        return lax.rem(self.x + 4 - d, 4)

    def ym(self, d):
        return lax.rem(self.y + 4 - d, 4)

    def to_x(self, d):
        return {'col': self.y, 'fsdp': lax.rem(self.x + d, 4) * 2 + self.c}

    def to_y(self, d):
        return {'col': lax.rem(self.y + d, 4), 'fsdp': self.x * 2 + self.c}

    def to_core(self):
        return {'col': self.y, 'fsdp': self.x * 2 + 1 - self.c}

    def to_z(self, d):
        return {'dp': lax.rem(self.z + d, 4)}


def rcopy(src, dst, ssem, rsem, dev):
    return pltpu.make_async_remote_copy(
        src_ref=src, dst_ref=dst, send_sem=ssem, recv_sem=rsem, device_id=dev, device_id_type=MESH)


def barrier(w):
    sem = pltpu.get_barrier_semaphore()
    devs = [w.to_core()] + [to(d) for d in OFFS for to in (w.to_x, w.to_y, w.to_z)]
    for dev in devs:
        pl.semaphore_signal(sem, inc=1, device_id=dev, device_id_type=MESH)
    pl.semaphore_wait(sem, len(devs))


class Gather:
    def __init__(self, w, buf, own_s, own_r, fa_s, fa_r, fb_s, fb_r, d_s, d_r):
        self.w, self.buf = w, buf
        self.own_s, self.own_r = own_s, own_r
        self.fa_s, self.fa_r, self.fb_s, self.fb_r = fa_s, fa_r, fb_s, fb_r
        self.d_s, self.d_r = d_s, d_r
        self.sent = []

    def piece(self, dx, dy, core=None):
        w = self.w
        return self.buf.at[w.ym(dy), w.xm(dx), w.c if core is None else core]

    def go(self, ref, ssem, rsem, dev):
        c = rcopy(ref, ref, ssem, rsem, dev)
        c.start()
        self.sent.append(c)

    def wait(self, ref, rsem):
        rcopy(ref, ref, rsem, rsem, self.w.to_core()).wait_recv()

    def share(self, dx, dy):
        self.go(self.piece(dx, dy), self.d_s.at[dx, dy], self.d_r.at[dx, dy], self.w.to_core())

    def start(self):
        me = self.piece(0, 0)
        for i, d in enumerate(OFFS):
            self.go(me, self.own_s.at[0, i], self.own_r.at[0, i], self.w.to_x(d))
            self.go(me, self.own_s.at[1, i], self.own_r.at[1, i], self.w.to_y(d))
        self.share(0, 0)

    def middle(self):
        w = self.w
        lo, hi = pl.ds(0, LA), pl.ds(LA, PK - LA)
        for i, d in enumerate(OFFS):
            p = self.piece(d, 0)
            self.wait(p, self.own_r.at[0, i])
            for j, e in enumerate(OFFS):
                self.go(p.at[:, lo], self.fa_s.at[i, j], self.fa_r.at[i, j], w.to_y(e))
            self.share(d, 0)
            p = self.piece(0, d)
            self.wait(p, self.own_r.at[1, i])
            for j, e in enumerate(OFFS):
                self.go(p.at[:, hi], self.fb_s.at[i, j], self.fb_r.at[i, j], w.to_x(e))
            self.share(0, d)

    def last(self):
        lo, hi = pl.ds(0, LA), pl.ds(LA, PK - LA)
        for i, dx in enumerate(OFFS):
            for j, dy in enumerate(OFFS):
                p = self.piece(dx, dy)
                self.wait(p.at[:, lo], self.fa_r.at[i, j])
                self.wait(p.at[:, hi], self.fb_r.at[j, i])
                self.share(dx, dy)

    def finish(self):
        for dx in range(4):
            for dy in range(4):
                self.wait(self.piece(dx, dy, 1 - self.w.c), self.d_r.at[dx, dy])

    def drain(self):
        for c in self.sent:
            c.wait_send()


def pack(dst, refs):
    for k, r in enumerate(refs):
        dst[:, 256 * k:256 * k + 256] = r[:, :256]
    rem = jnp.concatenate([r[:, 256:].astype(F32) for r in refs] + [jnp.zeros((SH, 32), F32)], axis=1)
    dst[:, 768:] = rem.astype(BF16)


def comm_kernel(wg, wu, wd, vg, vu, vd, g_hbm, gw_out, gv_out, dwn_out,
                gw, gv, gbuf, gt, rb0, cs, rb1a, rb1b, s1a, s1b, rb2a, rb2b, gz,
                ld_sem, st_sem,
                w0, w1, w2, w3, w4, w5, w6, w7, v0, v1, v2, v3, v4, v5, v6, v7,
                r0s, r0r, r1s, r1r, r2s, r2r, r3s, r3r):
    w = Where()
    load = pltpu.make_async_copy(g_hbm, gbuf, ld_sem)
    load.start()
    pack(gw.at[w.y, w.x, w.c], (wg, wu, wd))
    pack(gv.at[w.y, w.x, w.c], (vg, vu, vd))
    barrier(w)
    gather_w = Gather(w, gw, w0, w1, w2, w3, w4, w5, w6, w7)
    gather_v = Gather(w, gv, v0, v1, v2, v3, v4, v5, v6, v7)
    gather_w.start()

    load.wait()
    for m in range(7):
        if m < 6:
            blk = gbuf[m // 2, 128 * (m % 2):128 * (m % 2) + 128, :]
        else:
            blk = jnp.concatenate([gbuf[k, 256:, :] for k in range(3)] + [jnp.zeros((32, F), F32)], axis=0)
        t = blk.T
        for j in range(32):
            gt[j // 8, (j // 2) % 4, j % 2, :, 128 * m:128 * m + 128] = t[SH * j:SH * j + SH].astype(BF16)

    gather_w.middle()
    c0 = rcopy(gt.at[:, :, 1 - w.c], rb0, r0s, r0r, w.to_core())
    c0.start()
    gather_w.last()
    gather_w.finish()
    gather_w.drain()
    out_w = pltpu.make_async_copy(gw, gw_out, st_sem.at[0])
    out_w.start()
    gather_v.start()
    c0.wait()
    for y in range(4):
        for x in range(4):
            cs[y, x] = (gt[y, x, w.c].astype(F32) + rb0[y, x].astype(F32)).astype(BF16)
    sends = []
    lo, hi = pl.ds(0, LA), pl.ds(LA, PK - LA)
    for i, d in enumerate(OFFS):
        ca = rcopy(cs.at[:, lax.rem(w.x + d, 4), :, lo], rb1a.at[i], r1s.at[0, i], r1r.at[0, i], w.to_x(d))
        ca.start()
        cb = rcopy(cs.at[lax.rem(w.y + d, 4), :, :, hi], rb1b.at[i], r1s.at[1, i], r1r.at[1, i], w.to_y(d))
        cb.start()
        sends += [ca, cb]
    gather_v.middle()
    for c in sends:
        c.wait()
    for k in range(4):
        acc = cs[k, w.x, :, :LA].astype(F32)
        for i in range(3):
            acc += rb1a[i, k].astype(F32)
        s1a[k] = acc.astype(BF16)
        acc = cs[w.y, k, :, LA:].astype(F32)
        for i in range(3):
            acc += rb1b[i, k].astype(F32)
        s1b[k] = acc.astype(BF16)
    sends = []
    for i, d in enumerate(OFFS):
        ca = rcopy(s1a.at[lax.rem(w.y + d, 4)], rb2a.at[i], r2s.at[0, i], r2r.at[0, i], w.to_y(d))
        ca.start()
        cb = rcopy(s1b.at[lax.rem(w.x + d, 4)], rb2b.at[i], r2s.at[1, i], r2r.at[1, i], w.to_x(d))
        cb.start()
        sends += [ca, cb]
    gather_v.last()
    for c in sends:
        c.wait()
    acc = s1a[w.y].astype(F32)
    for i in range(3):
        acc += rb2a[i].astype(F32)
    gz[w.z, :, :LA] = acc.astype(BF16)
    acc = s1b[w.x].astype(F32)
    for i in range(3):
        acc += rb2b[i].astype(F32)
    gz[w.z, :, LA:] = acc.astype(BF16)
    gather_v.finish()
    sends = []
    for i, d in enumerate(OFFS):
        c = rcopy(gz.at[w.z], gz.at[w.z], r3s.at[i], r3r.at[i], w.to_z(d))
        c.start()
        sends.append(c)
    gather_v.drain()
    out_v = pltpu.make_async_copy(gv, gv_out, st_sem.at[1])
    out_v.start()
    for i, d in enumerate(OFFS):
        zm = gz.at[lax.rem(w.z + 4 - d, 4)]
        rcopy(zm, zm, r3s.at[i], r3r.at[i], w.to_core()).wait_recv()
    for c in sends:
        c.wait_send()
    tot = ((gz[0].astype(F32) + gz[1].astype(F32)) + gz[2].astype(F32)) + gz[3].astype(F32)
    for k in range(3):
        dwn_out[k, :, :256] = tot[:, 256 * k:256 * k + 256]
        dwn_out[k, :, 256:] = tot[:, 768 + 32 * k:800 + 32 * k]
    out_w.wait()
    out_v.wait()


def communicate(ws, vs, g):
    vmem = pl.BlockSpec(memory_space=pltpu.VMEM)
    hbm = pl.BlockSpec(memory_space=pl.ANY)
    dma = pltpu.SemaphoreType.DMA
    gsems = [dma((2, 3)), dma((2, 3)), dma((3, 3)), dma((3, 3)), dma((3, 3)), dma((3, 3)), dma((4, 4)), dma((4, 4))]
    full = (4, 4, 2, SH, PK)
    return pl.pallas_call(
        comm_kernel,
        out_shape=(jax.ShapeDtypeStruct(full, BF16), jax.ShapeDtypeStruct(full, BF16),
                   jax.ShapeDtypeStruct((3, SH, D), F32)),
        in_specs=[vmem] * 6 + [hbm],
        out_specs=(hbm, hbm, vmem),
        scratch_shapes=[
            pltpu.VMEM(full, BF16), pltpu.VMEM(full, BF16),
            pltpu.VMEM((3, D, F), F32), pltpu.VMEM(full, BF16),
            pltpu.VMEM((4, 4, SH, PK), BF16), pltpu.VMEM((4, 4, SH, PK), BF16),
            pltpu.VMEM((3, 4, SH, LA), BF16), pltpu.VMEM((3, 4, SH, PK - LA), BF16),
            pltpu.VMEM((4, SH, LA), BF16), pltpu.VMEM((4, SH, PK - LA), BF16),
            pltpu.VMEM((3, SH, LA), BF16), pltpu.VMEM((3, SH, PK - LA), BF16),
            pltpu.VMEM((4, SH, PK), BF16),
            dma, dma((2,)), *gsems, *gsems,
            dma, dma, dma((2, 3)), dma((2, 3)), dma((2, 3)), dma((2, 3)), dma((3,)), dma((3,)),
        ],
        compiler_params=pltpu.CompilerParams(collective_id=0, has_side_effects=True, vmem_limit_bytes=48 * 2**20),
        name="comm",
    )(*ws, *vs, g)


def mlp_kernel(xt, dyt, gw, gv, dxt, dw, vg, vu, vd, wcat, dcat):
    i = pl.program_id(0)

    @pl.when(i == 0)
    def _():
        rem = gw[:, 768:].T
        for k in range(2):
            wcat[:256, F * k:F * k + F] = gw[:, 256 * k:256 * k + 256].T
            wcat[256:, F * k:F * k + F] = rem[32 * k:32 * k + 32]
        rem = gv[:, 768:].T
        for k, o in enumerate((vg, vu, vd)):
            o[:256] = gv[:, 256 * k:256 * k + 256].T
            o[256:] = rem[32 * k:32 * k + 32]
        dw[...] = jnp.zeros_like(dw)

    dot = functools.partial(jnp.dot, preferred_element_type=F32)
    nt = lambda p, q: lax.dot_general(p, q, (((1,), (1,)), ((), ())), preferred_element_type=F32)
    x, dy = xt[...], dyt[...]
    zero = jnp.zeros((32, TB), BF16)
    wr = gw[:, 768:]

    def up(k, t):
        rem = [zero] * 4
        rem[k] = t[256:]
        return dot(gw[:, 256 * k:256 * k + 256], t[:256]) + dot(wr, jnp.concatenate(rem, axis=0))

    a = up(0, x)
    b = up(1, x)
    dh = up(2, dy)
    s = jax.nn.sigmoid(a)
    act = a * s
    h = (act * b).astype(BF16)
    dg = (dh * b * (s + act * (1.0 - s))).astype(BF16)
    du = (dh * act).astype(BF16)
    dcat[:F] = dg
    dcat[F:] = du
    dxt[...] = dot(wcat[...], dcat[...]).astype(BF16)
    dw[0] += nt(x, dg)
    dw[1] += nt(x, du)
    dw[2] += nt(dy, h)


def mlp(xt, dyt, gw, gv):
    full = lambda *s: pl.BlockSpec(s, lambda i: (0,) * len(s))
    tok = pl.BlockSpec((D, TB), lambda i: (0, i))
    return pl.pallas_call(
        mlp_kernel, grid=(T // TB,),
        out_shape=(jax.ShapeDtypeStruct((D, T), BF16), jax.ShapeDtypeStruct((3, D, F), F32),
                   *[jax.ShapeDtypeStruct((D, F), BF16)] * 3),
        in_specs=[tok, tok, full(F, PK), full(F, PK)],
        out_specs=(tok, full(3, D, F), full(D, F), full(D, F), full(D, F)),
        scratch_shapes=[pltpu.VMEM((D, 2 * F), BF16), pltpu.VMEM((2 * F, TB), BF16)],
        compiler_params=pltpu.CompilerParams(dimension_semantics=("arbitrary",), vmem_limit_bytes=48 * 2**20),
        name="mlp",
    )(xt, dyt, gw, gv)


def solution(mesh):
    def device_step(x_loc, dy_loc, w_gate, w_up, w_down, v_gate, v_up, v_down, g_next):
        gw, gv, dwn = communicate((w_gate.T, w_up.T, w_down), (v_gate.T, v_up.T, v_down), g_next[0])
        dxt, dw, vg, vu, vd = mlp(x_loc.T, dy_loc.T, gw.reshape(F, PK), gv.reshape(F, PK))
        return dxt.T, dwn.transpose(0, 2, 1), dw[None], vg, vu, vd.T

    row_spec = P(ALL_AXES, None)
    col_shard = P(None, FSDP_AXES)
    row_shard = P(FSDP_AXES, None)
    dev_spec = P(ALL_AXES, None, None, None)
    return jax.shard_map(
        device_step, mesh=mesh,
        in_specs=(row_spec, row_spec, col_shard, col_shard, row_shard, col_shard, col_shard, row_shard, dev_spec),
        out_specs=(row_spec, P(None, None, FSDP_AXES), dev_spec, P(), P(), P()),
        check_vma=False)
```
